128 devices in a mesh: expert: 64 (over z, y_lo, x, core), dp: 2 (over y_hi).
Axes of the slice: x: 4, y: 4 (y_hi: 2, y_lo: 2; y = y_hi * 2 + y_lo), z: 4, core: 2. Of those that a mesh axis runs over, the one named last changes fastest.
Arguments:
- tokens: bfloat16 [6144, 2880], P(('expert', 'dp')), may hold values from -6 to 6
- expert_ids: int32 [6144, 4], P(('expert', 'dp')), may hold values from 0 to 63, all different within a row; in each aligned block of 48 rows (0 to 47, 48 to 95, ...) at most 6 rows name the same one
- combine_int: int32 [6144, 4], P(('expert', 'dp')), may hold values from 8 to 63
- gate_weight: bfloat16 [64, 2880, 2880], P('expert', None, 'dp'), may hold values from -0.109375 to 0.109375
- up_weight: bfloat16 [64, 2880, 2880], P('expert', None, 'dp'), may hold values from -0.109375 to 0.109375
- down_weight: bfloat16 [64, 2880, 2880], P('expert', 'dp'), may hold values from -0.109375 to 0.109375
Outputs:
- mixed: bfloat16 [6144, 2880], P(('expert', 'dp'))
The draws below stay inside these ranges and needn't reach their ends.
Inputs may be any that keep to these rules, and one draw needn't show every extreme that they name: `expert_ids`: each row names 4 different experts; within the 48 rows of one device no expert is named by more than 6 rows, a bound that some block reaches.
All inputs are finite; a program needn't handle non-finite values.
Results may differ from the reference program's by a relative error of at most 0.0049.
Values may be sent and summed in bfloat16 or wider, within the bound.
No kernel may reach another device: no remote copies, remote signals or barrier semaphores. Data moves between devices by JAX's collectives and lax.ppermute only.
A program may use at most 128 MiB of HBM per device.

```python
import math
import jax
import jax.numpy as jnp
import numpy as np
from jax import lax

D = 2880
FF = 2880
TOP = 4
TOK_DEV = 48
EXPERTS = 64
CAP = 6
TOKENS = 6144


def touch_ends(drawn, key, least, top_value):
    extent = drawn.shape
    place = [jax.random.randint(jax.random.fold_in(key, axis), (), 0, extent[axis]) for axis in range(len(extent))]
    drawn = drawn.at[tuple(place)].set(least)
    longest = extent.index(max(extent))
    place[longest] = (place[longest] + 1) % extent[longest]
    return drawn.at[tuple(place)].set(top_value)


def steps_of(key, shape, cuts, low, largest):
    gain = 1.0
    for dim, blocks in cuts:
        draws = jax.random.uniform(jax.random.fold_in(jax.random.fold_in(key, 6), dim), (blocks,), jnp.float32, low / len(cuts), largest / len(cuts))
        gain = gain * jnp.repeat(jnp.exp(draws), shape[dim] // blocks).reshape((-1,) + (1,) * (len(shape) - 1 - dim))
    return gain


def deal_out(own_key, own, number, rows, amount, top, bound, lean):
    ranking = jax.random.permutation(own_key, amount)
    crowded, common = portions_of(amount, rows * top, bound, lean, True), portions_of(amount, rows * top, bound, lean, False)
    places = jnp.arange(amount)

    def named(tallies, offset_by):
        used = int((tallies > 0).sum())
        fixed = max(1, used // 4)
        passed = fixed + (places - fixed + offset_by * (used - fixed)) % max(1, amount - fixed)
        return jnp.zeros((amount,), jnp.int32).at[ranking[jnp.where(places < fixed, places, passed)]].set(jnp.asarray(tallies, jnp.int32))

    tallies = jnp.where(number % 4 == 0, named(crowded, number // 4), named(common, number - number // 4 - 1))
    mixed = jax.random.permutation(jax.random.fold_in(own, 3), amount)
    source_of, sink = mixed[0:amount // 2 * 2:2], mixed[1:amount // 2 * 2:2]
    margin = jnp.minimum(tallies[source_of] - 1, bound - tallies[sink]) // 2
    margin = jnp.where((source_of == ranking[0]) | (sink == ranking[0]) | (tallies[sink] == 0), 0, jnp.maximum(margin, 0))
    passed = jax.random.randint(jax.random.fold_in(own, 4), (amount // 2,), 0, 1 << 20) % (margin + 1)
    tallies = tallies.at[source_of].add(-passed).at[sink].add(passed)
    labels = jnp.searchsorted(jnp.cumsum(tallies), jnp.arange(rows * top), side="right").astype(jnp.int32)
    table = labels.reshape(top, rows).T
    table = table[jax.random.permutation(jax.random.fold_in(own, 1), rows)]
    offset_by = jax.random.randint(jax.random.fold_in(own, 2), (rows, 1), 0, top)
    return jnp.take_along_axis(table, (jnp.arange(top)[None, :] + offset_by) % top, axis=1)


def portions_of(amount, total, bound, slope, full):
    weights = [(1 << 20) // math.isqrt(standing ** slope) + 1 for standing in range(1, amount + 1)]
    largest = bound if full else min(bound, max(-(-total // amount), total * weights[0] // sum(weights)))
    least = 1 if total - largest >= amount - 1 else 0
    counts, rest = [largest] + [least] * (amount - 1), total - largest - least * (amount - 1)
    while rest > 0:
        free = [i for i in range(1, amount) if counts[i] < largest] or [i for i in range(1, amount) if counts[i] < bound]
        whole, budget = sum([weights[i] for i in free]), rest
        for i in free:
            extra = min(bound - counts[i], max(1, budget * weights[i] // whole), rest)
            counts[i] = counts[i] + extra
            rest = rest - extra
    return np.array(counts)


def normal_values(key, extent, scale, limit, pieces=(), kind=jnp.bfloat16):
    drawn = scale * jax.random.normal(key, extent, jnp.float32)
    if pieces:
        drawn = drawn * steps_of(key, extent, pieces, -0.22, 0.18)
    return jnp.clip(drawn, -limit, limit).astype(kind)


def setup_inputs(seed: int = 0) -> dict:
    key_list = jax.random.split(jax.random.key(seed), 7)
    tokens = normal_values(key_list[0], (TOKENS, D), 1.0, 6.0, ((0, 128),))
    expert_ids_keys = jax.random.split(jax.random.fold_in(key_list[1], 1), TOKENS // TOK_DEV)
    expert_ids_turns = jax.random.permutation(jax.random.fold_in(key_list[1], 3), TOKENS // TOK_DEV)
    expert_ids = jax.vmap(lambda own, number: deal_out(jax.random.fold_in(key_list[1], 2), own, number, TOK_DEV, EXPERTS, TOP, CAP, 2))(expert_ids_keys, expert_ids_turns).reshape((TOKENS, TOP))
    combine_int = touch_ends(jax.random.randint(key_list[2], (TOKENS, TOP), 8, 64), jax.random.fold_in(key_list[2], 1), 8, 63).astype(jnp.int32)
    gate_weight = normal_values(key_list[3], (EXPERTS, D, FF), D ** -0.5, 0.109375, ((0, 64), (2, 2)))
    up_weight = normal_values(key_list[4], (EXPERTS, D, FF), D ** -0.5, 0.109375, ((0, 64), (2, 2)))
    down_weight = normal_values(key_list[5], (EXPERTS, FF, D), FF ** -0.5, 0.109375, ((0, 64), (1, 2)))
    return {"tokens": tokens, "expert_ids": expert_ids, "combine_int": combine_int, "gate_weight": gate_weight, "up_weight": up_weight, "down_weight": down_weight}


def expert_rows(rows, gate_w, up_w, down_w):
    gate = jnp.dot(rows, gate_w, preferred_element_type=jnp.float32)
    up = jnp.dot(rows, up_w, preferred_element_type=jnp.float32)
    hidden = (gate * jax.nn.sigmoid(1.702 * gate) * (up + 1.0)).astype(jnp.bfloat16)
    return jnp.dot(hidden, down_w, preferred_element_type=jnp.float32)


def reference(tokens, expert_ids, combine_int, gate_weight, up_weight, down_weight):
    devices = TOKENS // TOK_DEV
    slots = devices * CAP
    weights = combine_int.astype(jnp.float32) / 32.0

    def one_expert(carry, index):
        hit = expert_ids == index
        chosen = jnp.any(hit, axis=1).astype(jnp.int32)
        scale = jnp.sum(jnp.where(hit, weights, jnp.zeros_like(weights)), axis=1)
        rank = jnp.cumsum(chosen.reshape(devices, TOK_DEV), axis=1) - 1
        places = (jnp.arange(devices, dtype=jnp.int32)[:, None] * CAP + rank).reshape(-1).astype(jnp.int32)
        places = jnp.where(chosen > 0, places, slots).astype(jnp.int32)
        rows = jnp.zeros((slots + 1, D), jnp.bfloat16).at[places].set(tokens)
        result = expert_rows(rows[:slots], gate_weight[index], up_weight[index], down_weight[index])
        picked = jnp.take(result, jnp.minimum(places, slots - 1), axis=0)
        return carry + scale[:, None] * picked, None

    start = jnp.zeros((TOKENS, D), jnp.float32)
    total, _ = lax.scan(one_expert, start, jnp.arange(EXPERTS, dtype=jnp.int32))
    return total.astype(jnp.bfloat16)
```

```python
import jax
import jax.numpy as jnp
from jax import lax
from jax.experimental import pallas as pl
from jax.experimental.pallas import tpu as pltpu
from jax.sharding import PartitionSpec as P

AXES = ("expert", "dp")
EXPERTS = 64
PARTS = 128
TOK = 48
TOP = 4
D = 2880
HID = 1440
HPAD = 1536
Q = 768
WIDTHS = (Q, Q, Q, D - 3 * Q)
GROUPS = ((0, 1, 2),)
BF = jnp.bfloat16
F32 = jnp.float32


def dot(a, b):
    return jnp.dot(a, b, preferred_element_type=F32)


def dot_nt(a, b):
    return lax.dot_general(a, b, (((1,), (1,)), ((), ())), preferred_element_type=F32)


def iota(shape, dim):
    return lax.broadcasted_iota(jnp.int32, shape, dim)


def ones_where(mask):
    return jnp.where(mask, jnp.ones(mask.shape, F32), jnp.zeros(mask.shape, F32)).astype(BF)


def spread(chosen):
    t = iota((TOK, 256), 0)
    c = iota((TOK, 256), 1) & 63
    return dot(chosen, ones_where(t == c)), dot(chosen, ones_where(t < c))


def pack_kernel(ids_ref, tok_ref, *refs):
    outs, tq_ref = refs[:-1], refs[-1]
    tq_ref[...] = jnp.zeros(tq_ref.shape, BF)
    for q in range(4):
        tq_ref[q * 64 : q * 64 + TOK, 0 : WIDTHS[q]] = tok_ref[:, q * Q : q * Q + WIDTHS[q]]
    rows = EXPERTS * 8
    expert = iota((rows, TOK), 0) >> 3
    hit = ids_ref[0:1, :] == expert
    for k in range(1, TOP):
        hit = hit | (ids_ref[k : k + 1, :] == expert)
    ch, rank = spread(ones_where(hit))
    row, col = iota((rows, 256), 0), iota((rows, 256), 1)
    fits = (((row >> 1) & 3) == (col >> 6)) & (ch > 0.5)
    parity = (row & 1).astype(F32)
    for group, out in zip(GROUPS, outs):
        for n, pair in enumerate(group):
            sel = ones_where(fits & (rank == parity + float(2 * pair)))
            val = dot(sel, tq_ref[...]).astype(BF).reshape(EXPERTS, 8, Q)
            for half in range(2):
                out[:, half, :, n * Q : (n + 1) * Q] = val


def mix_kernel(ids_ref, int_ref, out_ref):
    rows = PARTS * 8
    expert = iota((rows, TOK), 0) >> 4
    hit = ids_ref[0:1, :] == expert
    weight = jnp.where(hit, int_ref[0:1, :], 0)
    for k in range(1, TOP):
        now = ids_ref[k : k + 1, :] == expert
        weight = weight + jnp.where(now, int_ref[k : k + 1, :], 0)
        hit = hit | now
    ch, rank = spread(ones_where(hit))
    t = iota((TOK, 256), 0)
    c = iota((TOK, 256), 1) & 63
    scale = dot(weight.astype(F32).astype(BF), ones_where(t == c)) * (1.0 / 32.0)
    row, col = iota((rows, 256), 0), iota((rows, 256), 1)
    fits = (((row >> 1) & 3) == (col >> 6)) & (ch > 0.5)
    parity = (row & 1).astype(F32)
    for pair in range(3):
        mix = jnp.where(fits & (rank == parity + float(2 * pair)), scale, 0.0)
        out_ref[pair] = jnp.transpose(mix).astype(BF)


def mlp_kernel(pairs, x_ref, wg_hbm, wu_hbm, wd_hbm, out_ref, wg, wu, wd, x, hid, sems):
    blocks = [(i * 256, min(256, HID - i * 256)) for i in range(6)]
    copies = []
    for i, (at, size) in enumerate(blocks):
        for j, (src, dst) in enumerate(((wg_hbm, wg), (wu_hbm, wu))):
            copies.append(pltpu.make_async_copy(src.at[pl.ds(at, size), :], dst.at[pl.ds(at, size), :], sems.at[2 * i + j]))
    down = pltpu.make_async_copy(wd_hbm, wd.at[pl.ds(0, HID), :], sems.at[12])
    for c in copies:
        c.start()
    down.start()
    wg[HID:HPAD, :] = jnp.zeros((HPAD - HID, D), BF)
    wu[HID:HPAD, :] = jnp.zeros((HPAD - HID, D), BF)
    wd[HID:HPAD, :] = jnp.zeros((HPAD - HID, D), BF)

    to, fr = iota((256, 256), 0), iota((256, 256), 1)
    order = ones_where((((to >> 1) & 31) * 8 + (to >> 6) * 2 + (to & 1)) == fr)
    for n in range(pairs):
        for g in range(4):
            got = dot(order, x_ref[g * 256 : (g + 1) * 256, n * Q : (n + 1) * Q]).astype(BF)
            for q in range(4):
                x[n * 256 + g * 64 : n * 256 + (g + 1) * 64, q * Q : q * Q + WIDTHS[q]] = got[q * 64 : (q + 1) * 64, : WIDTHS[q]]

    for i in range(6):
        copies[2 * i].wait()
        copies[2 * i + 1].wait()
        gate = dot_nt(x[...], wg[i * 256 : (i + 1) * 256, :])
        up = dot_nt(x[...], wu[i * 256 : (i + 1) * 256, :])
        hid[:, i * 256 : (i + 1) * 256] = (gate * jax.nn.sigmoid(1.702 * gate) * (up + 1.0)).astype(BF)

    down.wait()
    back = ones_where((((fr >> 1) & 31) * 8 + (fr >> 6) * 2 + (fr & 1)) == to)
    for q in range(4):
        part = dot(hid[...], wd[:, q * Q : q * Q + WIDTHS[q]]).astype(BF)
        x[:, q * Q : q * Q + WIDTHS[q]] = part
    for n in range(pairs):
        for g in range(4):
            rows = slice(n * 256 + g * 64, n * 256 + (g + 1) * 64)
            full = [x[rows, q * Q : (q + 1) * Q] for q in range(3)]
            last = jnp.concatenate([x[rows, 3 * Q : D], jnp.zeros((64, 4 * Q - D), BF)], axis=1)
            stack = jnp.concatenate(full + [last], axis=0)
            out_ref[g * 256 : (g + 1) * 256, n * Q : (n + 1) * Q] = dot(back, stack).astype(BF)


def combine_kernel(mix_ref, *refs):
    ins, out_ref = refs[:-1], refs[-1]
    acc = None
    for group, ref in zip(GROUPS, ins):
        for n, pair in enumerate(group):
            part = dot(mix_ref[pair], ref[:, n * Q : (n + 1) * Q])
            acc = part if acc is None else acc + part
    for q in range(4):
        out_ref[:, q * Q : q * Q + WIDTHS[q]] = acc[q * 64 : q * 64 + TOK, : WIDTHS[q]].astype(BF)


def params(mib=56):
    return pltpu.CompilerParams(vmem_limit_bytes=mib * 1024 * 1024)


VM = pl.BlockSpec(memory_space=pltpu.VMEM)
HBM = pl.BlockSpec(memory_space=pl.ANY)


def mlp(arrived, gate_t, up_t, down, pairs):
    rows = 256 * pairs
    return pl.pallas_call(
        lambda *refs: mlp_kernel(pairs, *refs),
        out_shape=jax.ShapeDtypeStruct((PARTS * 8, pairs * Q), BF),
        in_specs=[VM, HBM, HBM, HBM],
        out_specs=VM,
        scratch_shapes=[
            pltpu.VMEM((HPAD, D), BF),
            pltpu.VMEM((HPAD, D), BF),
            pltpu.VMEM((HPAD, D), BF),
            pltpu.VMEM((rows, D), BF),
            pltpu.VMEM((rows, HPAD), BF),
            pltpu.SemaphoreType.DMA((13,)),
        ],
        compiler_params=params(),
        cost_estimate=pl.CostEstimate(
            flops=6 * rows * D * HID, transcendentals=rows * HID, bytes_accessed=6 * D * HID + 4 * rows * D
        ),
        name="mlp",
    )(arrived, gate_t, up_t, down)


def shards(tokens, expert_ids, combine_int, gate_weight, up_weight, down_weight):
    ids, ints = expert_ids.T, combine_int.T
    gate_t, up_t, down = gate_weight[0].T, up_weight[0].T, down_weight[0]
    sent = pl.pallas_call(
        pack_kernel,
        out_shape=[jax.ShapeDtypeStruct((EXPERTS, 2, 8, len(g) * Q), BF) for g in GROUPS],
        in_specs=[VM, VM],
        out_specs=[VM] * len(GROUPS),
        scratch_shapes=[pltpu.VMEM((256, Q), BF)],
        compiler_params=params(),
        name="pack",
    )(ids, tokens)
    mix = pl.pallas_call(
        mix_kernel,
        out_shape=jax.ShapeDtypeStruct((3, 256, PARTS * 8), BF),
        in_specs=[VM, VM],
        out_specs=VM,
        compiler_params=params(),
        name="mix",
    )(ids, ints)
    home = []
    for group, send in zip(GROUPS, sent):
        flat = send.reshape(PARTS * 8, len(group) * Q)
        arrived = lax.all_to_all(flat, AXES, 0, 0, tiled=True)
        result = mlp(arrived, gate_t, up_t, down, len(group))
        home.append(lax.all_to_all(result, AXES, 0, 0, tiled=True))
    return pl.pallas_call(
        combine_kernel,
        out_shape=jax.ShapeDtypeStruct((TOK, D), BF),
        in_specs=[VM] * (1 + len(GROUPS)),
        out_specs=VM,
        compiler_params=params(),
        name="combine",
    )(mix, *home)


def solution(mesh):
    return jax.shard_map(
        shards,
        mesh=mesh,
        in_specs=(
            P(("expert", "dp"), None),
            P(("expert", "dp"), None),
            P(("expert", "dp"), None),
            P("expert", None, "dp"),
            P("expert", None, "dp"),
            P("expert", "dp", None),
        ),
        out_specs=P(("expert", "dp"), None),
        check_vma=False,
    )
```

```python
import jax
import jax.numpy as jnp
from jax import lax
from jax.experimental import pallas as pl
from jax.experimental.pallas import tpu as pltpu
from jax.sharding import PartitionSpec as P

AXES = ("expert", "dp")
EXPERTS = 64
PARTS = 128
TOK = 48
TOP = 4
D = 2880
HID = 1440
HEAD = 2176
TAIL = D - HEAD
ROWS = PARTS * 6
GROUP = 32
BF = jnp.bfloat16
F32 = jnp.float32


def dot(a, b):
    return jnp.dot(a, b, preferred_element_type=F32)


def dot_nt(a, b):
    return lax.dot_general(a, b, (((1,), (1,)), ((), ())), preferred_element_type=F32)


def iota(shape, dim):
    return lax.broadcasted_iota(jnp.int32, shape, dim)


def ones_where(mask):
    return jnp.where(mask, jnp.ones(mask.shape, F32), jnp.zeros(mask.shape, F32)).astype(BF)


def pack_kernel(ids_ref, int_ref, tok_ref, out_ref, mix_ref, tok4):
    tok4[...] = jnp.zeros(tok4.shape, BF)
    tok4[0:TOK, :] = tok_ref[:, 0:HEAD]
    for j in range(3):
        tok4[(1 + j) * 64 : (1 + j) * 64 + TOK, j * TAIL : (j + 1) * TAIL] = tok_ref[:, HEAD:D]

    rows = EXPERTS * 8
    expert = iota((rows, TOK), 0) >> 3
    hit = ids_ref[0:1, :] == expert
    weight = jnp.where(hit, int_ref[0:1, :], 0)
    for k in range(1, TOP):
        now = ids_ref[k : k + 1, :] == expert
        weight = weight + jnp.where(now, int_ref[k : k + 1, :], 0)
        hit = hit | now
    hit = ones_where(hit)
    t, c = iota((TOK, 256), 0), iota((TOK, 256), 1) & 63
    same, before = ones_where(t == c), ones_where(t < c)
    chosen = dot(hit, same)
    rank = dot(hit, before)
    scale = dot(weight.astype(F32).astype(BF), same) * (1.0 / 32.0)
    row, block = iota((rows, 256), 0) & 7, iota((rows, 256), 1) >> 6
    head = jnp.where(row < 6, row, -1)
    tail = jnp.where(row < 6, -1, 3 * (row - 6) + block - 1)
    slot = jnp.where(block == 0, head, tail).astype(F32)
    fits = (chosen > 0.5) & (rank == slot)

    sent = dot(ones_where(fits), tok4[...]).astype(BF).reshape(EXPERTS, 8, HEAD)
    for half in range(2):
        out_ref[:, half, :, :] = sent
    mix = jnp.transpose(jnp.where(fits, scale, 0.0)).astype(BF)
    fr, to = iota((rows, PARTS * 8), 0), iota((rows, PARTS * 8), 1)
    mix_ref[...] = dot(mix, ones_where(fr == (to >> 4) * 8 + (to & 7))).astype(BF)


def arrival(r):
    at = ((r & 63) >> 1) * 8
    return at + jnp.where(r < 192, 3 * (r & 1) + (r >> 6), 6 + (r & 1))


def mlp_kernel(x_ref, wg_hbm, wu_hbm, wd_hbm, out_ref, wg, wu, wd, x, hid, y, sems):
    blocks = [(at, min(256, HID - at)) for at in range(0, HID, 256)]
    loads = []
    for i, (at, size) in enumerate(blocks):
        for j, (src, dst) in enumerate(((wg_hbm, wg), (wu_hbm, wu))):
            rows = pl.ds(at, size)
            loads.append(pltpu.make_async_copy(src.at[rows, :], dst.at[rows, :], sems.at[2 * i + j]))
    last = pltpu.make_async_copy(wd_hbm, wd, sems.at[2 * len(blocks)])
    for load in loads:
        load.start()
    last.start()

    a, b = iota((256, 256), 0), iota((256, 256), 1)
    order, back = ones_where(arrival(a) == b), ones_where(arrival(b) == a)
    for g in range(PARTS // GROUP):
        got = dot(order, x_ref[g * 256 : (g + 1) * 256, :]).astype(BF)
        x[g * 192 : (g + 1) * 192, 0:HEAD] = got[0:192]
        for j in range(3):
            x[g * 192 + j * 64 : g * 192 + (j + 1) * 64, HEAD:D] = got[192:256, j * TAIL : (j + 1) * TAIL]

    for i, (at, size) in enumerate(blocks):
        loads[2 * i].wait()
        loads[2 * i + 1].wait()
        gate = dot_nt(x[...], wg[at : at + size, :])
        up = dot_nt(x[...], wu[at : at + size, :])
        half = 0.5 * gate
        hid[:, at : at + size] = ((half + half * jnp.tanh(0.851 * gate)) * (up + 1.0)).astype(BF)

    last.wait()
    for at, size in ((0, 768), (768, 768), (1536, 640), (HEAD, TAIL)):
        part = dot(hid[...], wd[:, at : at + size]).astype(BF)
        for g in range(PARTS // GROUP):
            if at < HEAD:
                y[g * 256 : g * 256 + 192, at : at + size] = part[g * 192 : (g + 1) * 192]
            else:
                for j in range(3):
                    y[g * 256 + 192 : (g + 1) * 256, j * TAIL : (j + 1) * TAIL] = part[g * 192 + j * 64 : g * 192 + (j + 1) * 64]
    for g in range(PARTS // GROUP):
        y[g * 256 + 192 : (g + 1) * 256, 3 * TAIL : HEAD] = jnp.zeros((64, HEAD - 3 * TAIL), BF)
        out_ref[g * 256 : (g + 1) * 256, :] = dot(back, y[g * 256 : (g + 1) * 256, :]).astype(BF)


def combine_kernel(mix_ref, in_ref, out_ref):
    acc = dot(mix_ref[...], in_ref[...])
    out_ref[:, 0:HEAD] = acc[0:TOK].astype(BF)
    tail = acc[64 : 64 + TOK, 0:TAIL]
    for j in range(1, 3):
        tail = tail + acc[(1 + j) * 64 : (1 + j) * 64 + TOK, j * TAIL : (j + 1) * TAIL]
    out_ref[:, HEAD:D] = tail.astype(BF)


def params(mib):
    return pltpu.CompilerParams(vmem_limit_bytes=mib * 1024 * 1024)


VM = pl.BlockSpec(memory_space=pltpu.VMEM)
HBM = pl.BlockSpec(memory_space=pltpu.HBM)


def shards(tokens, expert_ids, combine_int, gate_weight, up_weight, down_weight):
    sent, mix = pl.pallas_call(
        pack_kernel,
        out_shape=[
            jax.ShapeDtypeStruct((EXPERTS, 2, 8, HEAD), BF),
            jax.ShapeDtypeStruct((256, PARTS * 8), BF),
        ],
        in_specs=[VM, VM, VM],
        out_specs=[VM, VM],
        scratch_shapes=[pltpu.VMEM((256, HEAD), BF)],
        compiler_params=params(16),
        name="pack",
    )(expert_ids.T, combine_int.T, tokens)
    arrived = lax.all_to_all(sent.reshape(PARTS * 8, HEAD), AXES, 0, 0, tiled=True)
    result = pl.pallas_call(
        mlp_kernel,
        out_shape=jax.ShapeDtypeStruct((PARTS * 8, HEAD), BF),
        in_specs=[VM, HBM, HBM, HBM],
        out_specs=VM,
        scratch_shapes=[
            pltpu.VMEM((HID, D), BF),
            pltpu.VMEM((HID, D), BF),
            pltpu.VMEM((HID, D), BF),
            pltpu.VMEM((ROWS, D), BF),
            pltpu.VMEM((ROWS, HID), BF),
            pltpu.VMEM((PARTS * 8, HEAD), BF),
            pltpu.SemaphoreType.DMA((13,)),
        ],
        compiler_params=params(44),
        cost_estimate=pl.CostEstimate(
            flops=6 * ROWS * D * HID, transcendentals=ROWS * HID, bytes_accessed=6 * D * HID + 4 * ROWS * D
        ),
        name="mlp",
    )(arrived, gate_weight[0].T, up_weight[0].T, down_weight[0])
    home = lax.all_to_all(result, AXES, 0, 0, tiled=True)
    return pl.pallas_call(
        combine_kernel,
        out_shape=jax.ShapeDtypeStruct((TOK, D), BF),
        in_specs=[VM, VM],
        out_specs=VM,
        compiler_params=params(12),
        name="combine",
    )(mix, home)


def solution(mesh):
    return jax.shard_map(
        shards,
        mesh=mesh,
        in_specs=(
            P(("expert", "dp"), None),
            P(("expert", "dp"), None),
            P(("expert", "dp"), None),
            P("expert", None, "dp"),
            P("expert", None, "dp"),
            P("expert", "dp", None),
        ),
        out_specs=P(("expert", "dp"), None),
        check_vma=False,
    )
```

```python
import jax
import jax.numpy as jnp
from jax import lax
from jax.experimental import pallas as pl
from jax.experimental.pallas import tpu as pltpu
from jax.sharding import PartitionSpec as P

AXES = ("expert", "dp")
EXPERTS = 64
PARTS = 128
TOK = 48
TOP = 4
D = 2880
HID = 1440
HEAD = 2176
TAIL = D - HEAD
ROWS = PARTS * 6
GROUP = 32
BF = jnp.bfloat16
F32 = jnp.float32


def dot(a, b):
    return jnp.dot(a, b, preferred_element_type=F32)


def dot_nt(a, b):
    return lax.dot_general(a, b, (((1,), (1,)), ((), ())), preferred_element_type=F32)


def iota(shape, dim):
    return lax.broadcasted_iota(jnp.int32, shape, dim)


def ones_where(mask):
    return jnp.where(mask, jnp.ones(mask.shape, F32), jnp.zeros(mask.shape, F32)).astype(BF)


def pack_kernel(code_ref, tok_ref, out_ref, mix_ref, tok4):
    tok4[...] = jnp.zeros(tok4.shape, BF)
    tok4[0:TOK, :] = tok_ref[:, 0:HEAD]
    for j in range(3):
        tok4[(1 + j) * 64 : (1 + j) * 64 + TOK, j * TAIL : (j + 1) * TAIL] = tok_ref[:, HEAD:D]

    rows = EXPERTS * 8
    expert = iota((rows, TOK), 0) >> 3
    hit, weight = None, None
    for k in range(TOP):
        code = code_ref[k : k + 1, :]
        now = (code >> 6) == expert
        held = jnp.where(now, code & 63, 0)
        hit = now if hit is None else hit | now
        weight = held if weight is None else weight + held
    hit = ones_where(hit)
    t, c = iota((TOK, 256), 0), iota((TOK, 256), 1) & 63
    same, before = ones_where(t == c), ones_where(t < c)
    chosen = dot(hit, same)
    rank = dot(hit, before)
    scale = dot(weight.astype(F32).astype(BF), same) * (1.0 / 32.0)
    row, block = iota((rows, 256), 0) & 7, iota((rows, 256), 1) >> 6
    head = jnp.where(row < 6, row, -1)
    tail = jnp.where(row < 6, -1, 3 * (row - 6) + block - 1)
    slot = jnp.where(block == 0, head, tail).astype(F32)
    fits = (chosen > 0.5) & (rank == slot)

    sent = dot(ones_where(fits), tok4[...]).astype(BF).reshape(EXPERTS, 8, HEAD)
    for half in range(2):
        out_ref[:, half, :, :] = sent
    mix = jnp.transpose(jnp.where(fits, scale, 0.0)).astype(BF)
    fr, to = iota((rows, PARTS * 8), 0), iota((rows, PARTS * 8), 1)
    both = dot(mix, ones_where(fr == (to >> 4) * 8 + (to & 7))).astype(BF)
    for j in range(4):
        mix_ref[j * TOK : (j + 1) * TOK, :] = both[j * 64 : j * 64 + TOK]


def arrival(r):
    at = ((r & 63) >> 1) * 8
    return at + jnp.where(r < 192, 3 * (r & 1) + (r >> 6), 6 + (r & 1))


def mlp_kernel(x_ref, wg, wu_hbm, wd_hbm, out_ref, wu, wd, first, x, hid, y, sems):
    loads = [
        pltpu.make_async_copy(src, dst, sems.at[i])
        for i, (src, dst) in enumerate(((wu_hbm, wu), (wd_hbm, wd)))
    ]
    for load in loads:
        load.start()

    a, b = iota((256, 256), 0), iota((256, 256), 1)
    order, back = ones_where(arrival(a) == b), ones_where(arrival(b) == a)
    for g in range(PARTS // GROUP):
        got = dot(order, x_ref[g * 256 : (g + 1) * 256, :]).astype(BF)
        x[g * 192 : (g + 1) * 192, 0:HEAD] = got[0:192]
        for j in range(3):
            x[g * 192 + j * 64 : g * 192 + (j + 1) * 64, HEAD:D] = got[192:256, j * TAIL : (j + 1) * TAIL]

    def gate_of(at, size):
        return dot_nt(x[...], wg[at : at + size, :])

    first[...] = gate_of(0, 512)
    loads[0].wait()
    for at in range(0, HID, 256):
        size = min(256, HID - at)
        gate = first[:, at : at + size] if at < 512 else gate_of(at, size)
        up = dot_nt(x[...], wu[at : at + size, :])
        half = 0.5 * gate
        hid[:, at : at + size] = ((half + half * jnp.tanh(0.851 * gate)) * (up + 1.0)).astype(BF)

    loads[1].wait()
    for at, size in ((0, 768), (768, 768), (1536, 640), (HEAD, TAIL)):
        part = dot(hid[...], wd[:, at : at + size]).astype(BF)
        for g in range(PARTS // GROUP):
            if at < HEAD:
                y[g * 256 : g * 256 + 192, at : at + size] = part[g * 192 : (g + 1) * 192]
            else:
                for j in range(3):
                    y[g * 256 + 192 : (g + 1) * 256, j * TAIL : (j + 1) * TAIL] = part[g * 192 + j * 64 : g * 192 + (j + 1) * 64]
    for g in range(PARTS // GROUP):
        y[g * 256 + 192 : (g + 1) * 256, 3 * TAIL : HEAD] = jnp.zeros((64, HEAD - 3 * TAIL), BF)
        out_ref[g * 256 : (g + 1) * 256, :] = dot(back, y[g * 256 : (g + 1) * 256, :]).astype(BF)


def combine_kernel(mix_ref, in_ref, out_ref):
    acc = dot(mix_ref[...], in_ref[...])
    out_ref[:, 0:HEAD] = acc[0:TOK].astype(BF)
    tail = acc[TOK : 2 * TOK, 0:TAIL]
    for j in range(1, 3):
        tail = tail + acc[(1 + j) * TOK : (2 + j) * TOK, j * TAIL : (j + 1) * TAIL]
    out_ref[:, HEAD:D] = tail.astype(BF)


def params(mib):
    return pltpu.CompilerParams(vmem_limit_bytes=mib * 1024 * 1024)


VM = pl.BlockSpec(memory_space=pltpu.VMEM)
HBM = pl.BlockSpec(memory_space=pltpu.HBM)


def shards(tokens, expert_ids, combine_int, gate_weight, up_weight, down_weight):
    sent, mix = pl.pallas_call(
        pack_kernel,
        out_shape=[
            jax.ShapeDtypeStruct((EXPERTS, 2, 8, HEAD), BF),
            jax.ShapeDtypeStruct((4 * TOK, PARTS * 8), BF),
        ],
        in_specs=[VM, VM],
        out_specs=[VM, VM],
        scratch_shapes=[pltpu.VMEM((256, HEAD), BF)],
        compiler_params=params(16),
        name="pack",
    )((expert_ids * 64 + combine_int).T, tokens)
    arrived = lax.all_to_all(sent.reshape(PARTS * 8, HEAD), AXES, 0, 0, tiled=True)
    result = pl.pallas_call(
        mlp_kernel,
        out_shape=jax.ShapeDtypeStruct((PARTS * 8, HEAD), BF),
        in_specs=[VM, VM, HBM, HBM],
        out_specs=VM,
        scratch_shapes=[
            pltpu.VMEM((HID, D), BF),
            pltpu.VMEM((HID, D), BF),
            pltpu.VMEM((ROWS, 512), F32),
            pltpu.VMEM((ROWS, D), BF),
            pltpu.VMEM((ROWS, HID), BF),
            pltpu.VMEM((PARTS * 8, HEAD), BF),
            pltpu.SemaphoreType.DMA((2,)),
        ],
        compiler_params=params(37),
        cost_estimate=pl.CostEstimate(
            flops=6 * ROWS * D * HID, transcendentals=ROWS * HID, bytes_accessed=6 * D * HID + 4 * ROWS * D
        ),
        name="mlp",
    )(arrived, gate_weight[0].T, up_weight[0].T, down_weight[0])
    home = lax.all_to_all(result, AXES, 0, 0, tiled=True)
    return pl.pallas_call(
        combine_kernel,
        out_shape=jax.ShapeDtypeStruct((TOK, D), BF),
        in_specs=[VM, VM],
        out_specs=VM,
        compiler_params=params(12),
        name="combine",
    )(mix, home)


def solution(mesh):
    return jax.shard_map(
        shards,
        mesh=mesh,
        in_specs=(
            P(("expert", "dp"), None),
            P(("expert", "dp"), None),
            P(("expert", "dp"), None),
            P("expert", None, "dp"),
            P("expert", None, "dp"),
            P("expert", "dp", None),
        ),
        out_specs=P(("expert", "dp"), None),
        check_vma=False,
    )
```

```python
import jax
import jax.numpy as jnp
from jax import lax
from jax.experimental import pallas as pl
from jax.experimental.pallas import tpu as pltpu
from jax.sharding import Mesh, PartitionSpec as P

AXES = ("z", "y", "x", "core", "half")
ORDER = ("half", "core", "y", "x", "z")
EXPERTS = 64
PARTS = 128
TOK = 48
TOP = 4
D = 2880
HID = 1440
HEAD = 2176
TAIL = D - HEAD
ROWS = PARTS * 6
GROUP = 32
BF = jnp.bfloat16
F32 = jnp.float32


def dot(a, b):
    return jnp.dot(a, b, preferred_element_type=F32)


def dot_nt(a, b):
    return lax.dot_general(a, b, (((1,), (1,)), ((), ())), preferred_element_type=F32)


def iota(shape, dim):
    return lax.broadcasted_iota(jnp.int32, shape, dim)


def ones_where(mask):
    return jnp.where(mask, jnp.ones(mask.shape, F32), jnp.zeros(mask.shape, F32)).astype(BF)


def pack_kernel(code_ref, tok_ref, out_ref, mix_ref, tok4):
    tok4[...] = jnp.zeros(tok4.shape, BF)
    tok4[0:TOK, :] = tok_ref[:, 0:HEAD]
    for j in range(3):
        tok4[(1 + j) * 64 : (1 + j) * 64 + TOK, j * TAIL : (j + 1) * TAIL] = tok_ref[:, HEAD:D]

    rows = EXPERTS * 8
    place = iota((rows, TOK), 0) >> 3
    expert = ((place & 3) << 4) | ((place & 16) >> 1) | ((place & 12) >> 1) | (place >> 5)
    hit, weight = None, None
    for k in range(TOP):
        code = code_ref[k : k + 1, :]
        now = (code >> 6) == expert
        held = jnp.where(now, code & 63, 0)
        hit = now if hit is None else hit | now
        weight = held if weight is None else weight + held
    hit = ones_where(hit)
    t, c = iota((TOK, 256), 0), iota((TOK, 256), 1) & 63
    same, before = ones_where(t == c), ones_where(t < c)
    chosen = dot(hit, same)
    rank = dot(hit, before)
    scale = dot(weight.astype(F32).astype(BF), same) * (1.0 / 32.0)
    row, block = iota((rows, 256), 0) & 7, iota((rows, 256), 1) >> 6
    head = jnp.where(row < 6, row, -1)
    tail = jnp.where(row < 6, -1, 3 * (row - 6) + block - 1)
    slot = jnp.where(block == 0, head, tail).astype(F32)
    fits = (chosen > 0.5) & (rank == slot)

    sent = dot(ones_where(fits), tok4[...]).astype(BF).reshape(EXPERTS, 8, HEAD)
    for half in range(2):
        out_ref[half] = sent
    mix = jnp.transpose(jnp.where(fits, scale, 0.0)).astype(BF)
    for j in range(4):
        mix_ref[j * TOK : (j + 1) * TOK, :] = mix[j * 64 : j * 64 + TOK]


def arrival(r):
    at = ((r & 63) >> 1) * 8
    return at + jnp.where(r < 192, 3 * (r & 1) + (r >> 6), 6 + (r & 1))


def mlp_kernel(x_ref, wg, wu_hbm, wd_hbm, out_ref, wu, wd, first, x, hid, y, sems):
    loads = [
        pltpu.make_async_copy(src, dst, sems.at[i])
        for i, (src, dst) in enumerate(((wu_hbm, wu), (wd_hbm, wd)))
    ]
    for load in loads:
        load.start()

    a, b = iota((256, 256), 0), iota((256, 256), 1)
    order, back = ones_where(arrival(a) == b), ones_where(arrival(b) == a)
    for g in range(PARTS // GROUP):
        got = dot(order, x_ref[g * 256 : (g + 1) * 256, :]).astype(BF)
        x[g * 192 : (g + 1) * 192, 0:HEAD] = got[0:192]
        for j in range(3):
            x[g * 192 + j * 64 : g * 192 + (j + 1) * 64, HEAD:D] = got[192:256, j * TAIL : (j + 1) * TAIL]

    def gate_of(at, size):
        return dot_nt(x[...], wg[at : at + size, :])

    first[...] = gate_of(0, 512)
    loads[0].wait()
    for at in range(0, HID, 256):
        size = min(256, HID - at)
        gate = first[:, at : at + size] if at < 512 else gate_of(at, size)
        up = dot_nt(x[...], wu[at : at + size, :])
        half = 0.5 * gate
        hid[:, at : at + size] = ((half + half * jnp.tanh(0.851 * gate)) * (up + 1.0)).astype(BF)

    loads[1].wait()
    for at, size in ((0, 768), (768, 768), (1536, 640), (HEAD, TAIL)):
        part = dot(hid[...], wd[:, at : at + size]).astype(BF)
        for g in range(PARTS // GROUP):
            if at < HEAD:
                y[g * 256 : g * 256 + 192, at : at + size] = part[g * 192 : (g + 1) * 192]
            else:
                for j in range(3):
                    y[g * 256 + 192 : (g + 1) * 256, j * TAIL : (j + 1) * TAIL] = part[g * 192 + j * 64 : g * 192 + (j + 1) * 64]
    for g in range(PARTS // GROUP):
        y[g * 256 + 192 : (g + 1) * 256, 3 * TAIL : HEAD] = jnp.zeros((64, HEAD - 3 * TAIL), BF)
        out_ref[g * 256 : (g + 1) * 256, :] = dot(back, y[g * 256 : (g + 1) * 256, :]).astype(BF)


def combine_kernel(mix_ref, in_ref, out_ref):
    acc = dot(mix_ref[...], in_ref[0 : EXPERTS * 8, :]) + dot(mix_ref[...], in_ref[EXPERTS * 8 :, :])
    out_ref[:, 0:HEAD] = acc[0:TOK].astype(BF)
    tail = acc[TOK : 2 * TOK, 0:TAIL]
    for j in range(1, 3):
        tail = tail + acc[(1 + j) * TOK : (2 + j) * TOK, j * TAIL : (j + 1) * TAIL]
    out_ref[:, HEAD:D] = tail.astype(BF)


def params(mib):
    return pltpu.CompilerParams(vmem_limit_bytes=mib * 1024 * 1024)


VM = pl.BlockSpec(memory_space=pltpu.VMEM)
HBM = pl.BlockSpec(memory_space=pltpu.HBM)


def shards(tokens, expert_ids, combine_int, gate_weight, up_weight, down_weight):
    sent, mix = pl.pallas_call(
        pack_kernel,
        out_shape=[
            jax.ShapeDtypeStruct((2, EXPERTS, 8, HEAD), BF),
            jax.ShapeDtypeStruct((4 * TOK, EXPERTS * 8), BF),
        ],
        in_specs=[VM, VM],
        out_specs=[VM, VM],
        scratch_shapes=[pltpu.VMEM((256, HEAD), BF)],
        compiler_params=params(16),
        name="pack",
    )((expert_ids * 64 + combine_int).T, tokens)
    arrived = lax.all_to_all(sent.reshape(PARTS * 8, HEAD), ORDER, 0, 0, tiled=True)
    result = pl.pallas_call(
        mlp_kernel,
        out_shape=jax.ShapeDtypeStruct((PARTS * 8, HEAD), BF),
        in_specs=[VM, VM, HBM, HBM],
        out_specs=VM,
        scratch_shapes=[
            pltpu.VMEM((HID, D), BF),
            pltpu.VMEM((HID, D), BF),
            pltpu.VMEM((ROWS, 512), F32),
            pltpu.VMEM((ROWS, D), BF),
            pltpu.VMEM((ROWS, HID), BF),
            pltpu.VMEM((PARTS * 8, HEAD), BF),
            pltpu.SemaphoreType.DMA((2,)),
        ],
        compiler_params=params(37),
        cost_estimate=pl.CostEstimate(
            flops=6 * ROWS * D * HID, transcendentals=ROWS * HID, bytes_accessed=6 * D * HID + 4 * ROWS * D
        ),
        name="mlp",
    )(arrived, gate_weight[0].T, up_weight[0].T, down_weight[0])
    home = lax.all_to_all(result, ORDER, 0, 0, tiled=True)
    return pl.pallas_call(
        combine_kernel,
        out_shape=jax.ShapeDtypeStruct((TOK, D), BF),
        in_specs=[VM, VM],
        out_specs=VM,
        compiler_params=params(12),
        name="combine",
    )(mix, home)


def solution(mesh):
    fine = Mesh(mesh.devices.reshape(4, 2, 4, 2, 2), AXES)
    return jax.shard_map(
        shards,
        mesh=fine,
        in_specs=(
            P(AXES, None),
            P(AXES, None),
            P(AXES, None),
            P(AXES[:4], None, AXES[4]),
            P(AXES[:4], None, AXES[4]),
            P(AXES[:4], AXES[4], None),
        ),
        out_specs=P(AXES, None),
        check_vma=False,
    )
```

```python
import jax
import jax.numpy as jnp
from jax import lax
from jax.experimental import pallas as pl
from jax.experimental.pallas import tpu as pltpu
from jax.sharding import Mesh, PartitionSpec as P

AXES = ("z", "y", "x", "core", "half")
ORDER = ("half", "core", "y", "x", "z")
EXPERTS = 64
PARTS = 128
TOK = 48
TOP = 4
D = 2880
HID = 1440
HEAD = 2176
TAIL = D - HEAD
ROWS = PARTS * 6
GROUP = 32
BF = jnp.bfloat16
F32 = jnp.float32


def dot(a, b):
    return jnp.dot(a, b, preferred_element_type=F32)


def dot_nt(a, b):
    return lax.dot_general(a, b, (((1,), (1,)), ((), ())), preferred_element_type=F32)


def iota(shape, dim):
    return lax.broadcasted_iota(jnp.int32, shape, dim)


def ones_where(mask):
    return jnp.where(mask, jnp.ones(mask.shape, F32), jnp.zeros(mask.shape, F32)).astype(BF)


def routes(code_ref):
    rows = EXPERTS * 8
    place = iota((rows, TOK), 0) >> 3
    expert = ((place & 3) << 4) | ((place & 16) >> 1) | ((place & 12) >> 1) | (place >> 5)
    hit, weight = None, None
    for k in range(TOP):
        code = code_ref[k : k + 1, :]
        now = (code >> 6) == expert
        held = jnp.where(now, code & 63, 0)
        hit = now if hit is None else hit | now
        weight = held if weight is None else weight + held
    hit = ones_where(hit)
    t, c = iota((TOK, 256), 0), iota((TOK, 256), 1) & 63
    same, before = ones_where(t == c), ones_where(t < c)
    chosen = dot(hit, same)
    rank = dot(hit, before)
    scale = dot(weight.astype(F32).astype(BF), same) * (1.0 / 32.0)
    row, block = iota((rows, 256), 0) & 7, iota((rows, 256), 1) >> 6
    head = jnp.where(row < 6, row, -1)
    tail = jnp.where(row < 6, -1, 3 * (row - 6) + block - 1)
    slot = jnp.where(block == 0, head, tail).astype(F32)
    fits = (chosen > 0.5) & (rank == slot)
    return fits, scale


def pack_kernel(code_ref, tok_ref, out_ref, tok4):
    tok4[...] = jnp.zeros(tok4.shape, BF)
    tok4[0:TOK, :] = tok_ref[:, 0:HEAD]
    for j in range(3):
        tok4[(1 + j) * 64 : (1 + j) * 64 + TOK, j * TAIL : (j + 1) * TAIL] = tok_ref[:, HEAD:D]

    fits, _ = routes(code_ref)
    sent = dot(ones_where(fits), tok4[...]).astype(BF).reshape(EXPERTS, 8, HEAD)
    for half in range(2):
        out_ref[half] = sent


def arrival(r):
    at = ((r & 63) >> 1) * 8
    return at + jnp.where(r < 192, 3 * (r & 1) + (r >> 6), 6 + (r & 1))


def mlp_kernel(x_ref, code_ref, wg, wu_hbm, wd_hbm, out_ref, mix_ref, wu, wd, first, x, hid, y, sems):
    loads = [
        pltpu.make_async_copy(src, dst, sems.at[i])
        for i, (src, dst) in enumerate(((wu_hbm, wu), (wd_hbm, wd)))
    ]
    for load in loads:
        load.start()

    a, b = iota((256, 256), 0), iota((256, 256), 1)
    order, back = ones_where(arrival(a) == b), ones_where(arrival(b) == a)
    for g in range(PARTS // GROUP):
        got = dot(order, x_ref[g * 256 : (g + 1) * 256, :]).astype(BF)
        x[g * 192 : (g + 1) * 192, 0:HEAD] = got[0:192]
        for j in range(3):
            x[g * 192 + j * 64 : g * 192 + (j + 1) * 64, HEAD:D] = got[192:256, j * TAIL : (j + 1) * TAIL]

    def gate_of(at, size):
        return dot_nt(x[...], wg[at : at + size, :])

    first[...] = gate_of(0, 512)
    fits, scale = routes(code_ref)
    mix = jnp.transpose(jnp.where(fits, scale, 0.0)).astype(BF)
    for j in range(4):
        mix_ref[j * TOK : (j + 1) * TOK, :] = mix[j * 64 : j * 64 + TOK]
    loads[0].wait()
    for at in range(0, HID, 256):
        size = min(256, HID - at)
        gate = first[:, at : at + size] if at < 512 else gate_of(at, size)
        up = dot_nt(x[...], wu[at : at + size, :])
        half = 0.5 * gate
        hid[:, at : at + size] = ((half + half * jnp.tanh(0.851 * gate)) * (up + 1.0)).astype(BF)

    loads[1].wait()
    for at, size in ((0, 768), (768, 768), (1536, 640), (HEAD, TAIL)):
        part = dot(hid[...], wd[:, at : at + size]).astype(BF)
        for g in range(PARTS // GROUP):
            if at < HEAD:
                y[g * 256 : g * 256 + 192, at : at + size] = part[g * 192 : (g + 1) * 192]
            else:
                for j in range(3):
                    y[g * 256 + 192 : (g + 1) * 256, j * TAIL : (j + 1) * TAIL] = part[g * 192 + j * 64 : g * 192 + (j + 1) * 64]
    for g in range(PARTS // GROUP):
        y[g * 256 + 192 : (g + 1) * 256, 3 * TAIL : HEAD] = jnp.zeros((64, HEAD - 3 * TAIL), BF)
        out_ref[g * 256 : (g + 1) * 256, :] = dot(back, y[g * 256 : (g + 1) * 256, :]).astype(BF)


def combine_kernel(mix_ref, in_ref, out_ref):
    acc = dot(mix_ref[...], in_ref[0 : EXPERTS * 8, :]) + dot(mix_ref[...], in_ref[EXPERTS * 8 :, :])
    out_ref[:, 0:HEAD] = acc[0:TOK].astype(BF)
    tail = acc[TOK : 2 * TOK, 0:TAIL]
    for j in range(1, 3):
        tail = tail + acc[(1 + j) * TOK : (2 + j) * TOK, j * TAIL : (j + 1) * TAIL]
    out_ref[:, HEAD:D] = tail.astype(BF)


def params(mib):
    return pltpu.CompilerParams(vmem_limit_bytes=mib * 1024 * 1024)


VM = pl.BlockSpec(memory_space=pltpu.VMEM)
HBM = pl.BlockSpec(memory_space=pltpu.HBM)


def shards(tokens, expert_ids, combine_int, gate_weight, up_weight, down_weight):
    code = (expert_ids * 64 + combine_int).T
    sent = pl.pallas_call(
        pack_kernel,
        out_shape=jax.ShapeDtypeStruct((2, EXPERTS, 8, HEAD), BF),
        in_specs=[VM, VM],
        out_specs=VM,
        scratch_shapes=[pltpu.VMEM((256, HEAD), BF)],
        compiler_params=params(16),
        name="pack",
    )(code, tokens)
    arrived = lax.all_to_all(sent.reshape(PARTS * 8, HEAD), ORDER, 0, 0, tiled=True)
    result, mix = pl.pallas_call(
        mlp_kernel,
        out_shape=[
            jax.ShapeDtypeStruct((PARTS * 8, HEAD), BF),
            jax.ShapeDtypeStruct((4 * TOK, EXPERTS * 8), BF),
        ],
        in_specs=[VM, VM, VM, HBM, HBM],
        out_specs=[VM, VM],
        scratch_shapes=[
            pltpu.VMEM((HID, D), BF),
            pltpu.VMEM((HID, D), BF),
            pltpu.VMEM((ROWS, 512), F32),
            pltpu.VMEM((ROWS, D), BF),
            pltpu.VMEM((ROWS, HID), BF),
            pltpu.VMEM((PARTS * 8, HEAD), BF),
            pltpu.SemaphoreType.DMA((2,)),
        ],
        compiler_params=params(37),
        cost_estimate=pl.CostEstimate(
            flops=6 * ROWS * D * HID, transcendentals=ROWS * HID, bytes_accessed=6 * D * HID + 4 * ROWS * D
        ),
        name="mlp",
    )(arrived, code, gate_weight[0].T, up_weight[0].T, down_weight[0])
    home = lax.all_to_all(result, ORDER, 0, 0, tiled=True)
    return pl.pallas_call(
        combine_kernel,
        out_shape=jax.ShapeDtypeStruct((TOK, D), BF),
        in_specs=[VM, VM],
        out_specs=VM,
        compiler_params=params(12),
        name="combine",
    )(mix, home)


def solution(mesh):
    fine = Mesh(mesh.devices.reshape(4, 2, 4, 2, 2), AXES)
    return jax.shard_map(
        shards,
        mesh=fine,
        in_specs=(
            P(AXES, None),
            P(AXES, None),
            P(AXES, None),
            P(AXES[:4], None, AXES[4]),
            P(AXES[:4], None, AXES[4]),
            P(AXES[:4], AXES[4], None),
        ),
        out_specs=P(AXES, None),
        check_vma=False,
    )
```
